32 devices in a mesh: cz: 4 (over z), cy: 2 (over y), cx: 4 (over x, core).
Axes of the slice: x: 2, y: 2, z: 4, core: 2. Of those that a mesh axis runs over, the one named last changes fastest.
Arguments:
- x: bfloat16 [1024, 4096], P(('cx', 'cz'), 'cy')
- w1: bfloat16 [4096, 16384], P('cy', ('cz', 'cx'))
- w2: bfloat16 [16384, 4096], P('cz', ('cy', 'cx'))
Outputs:
- output: bfloat16 [1024, 4096], P(('cx', 'cz'), 'cy')
All inputs are finite; a program needn't handle non-finite values.
Results may differ from the reference program's by a relative error of at most 0.0115307.
Values are sent between devices in bfloat16 or wider.
A program may use at most 1 GiB of HBM per device.

```python
import jax
import jax.numpy as jnp

N = 1024
D = 4096
F = 16384


def setup_inputs(seed: int = 0) -> dict:
    k1, k2, k3 = jax.random.split(jax.random.PRNGKey(seed), 3)
    x = jax.random.normal(k1, (N, D), jnp.float32)
    w1 = jax.random.normal(k2, (D, F), jnp.float32) * D ** -0.5
    w2 = jax.random.normal(k3, (F, D), jnp.float32) * F ** -0.5
    return {"x": x.astype(jnp.bfloat16), "w1": w1.astype(jnp.bfloat16), "w2": w2.astype(jnp.bfloat16)}


def reference(x, w1, w2):
    c = jnp.dot(x, w1, preferred_element_type=jnp.float32).astype(jnp.bfloat16)
    h = jax.nn.gelu(c.astype(jnp.float32), approximate=True).astype(jnp.bfloat16)
    return jnp.dot(h, w2, preferred_element_type=jnp.float32).astype(jnp.bfloat16)
```

```python
import math

import jax
import jax.numpy as jnp
from jax import lax
from jax.experimental import pallas as pl
from jax.experimental.pallas import tpu as pltpu
from jax.sharding import PartitionSpec as P

MESH = pl.DeviceIdType.MESH
ROWS = 64
HALF = ROWS // 2
BLOCKS = 16
LEAD = 2


def kernel(x_hbm, w1_hbm, w2_hbm, out_ref, xg, w1, w2, cp, crv, hg, zp, zu, zd, fb, ab, ld,
           x_xs, x_xr, x_ds, x_dr, x_us, x_ur, x_ns, x_nr, cs, cr, hys, hyr, hxs, hxr, gxs, gxr,
           d0s, d0r, d1s, d1r, zs, zur, znr, a_s, a_r):
    z, y, cx = lax.axis_index("cz"), lax.axis_index("cy"), lax.axis_index("cx")
    core = cx % 2
    xp = (cx + 2) % 4
    sib = cx + 1 - 2 * core
    sibxp = (sib + 2) % 4
    dev_y = (z, 1 - y, cx)
    dev_x = (z, y, xp)
    dev_s = (z, y, sib)
    dev_up = ((z + 1) % 4, y, cx)
    dev_dn = ((z + 3) % 4, y, cx)
    width = w1.shape[1]

    loads = [pltpu.make_async_copy(x_hbm, xg.at[z * 4 + cx], ld.at[0]),
             pltpu.make_async_copy(w1_hbm, w1, ld.at[1]),
             pltpu.make_async_copy(w2_hbm, w2, ld.at[2])]
    for load in loads:
        load.start()

    barrier = pltpu.get_barrier_semaphore()
    for dev in (dev_y, dev_x, dev_s, (z, y, sibxp)):
        pl.semaphore_signal(barrier, inc=1, device_id=dev, device_id_type=MESH)

    @pl.when(z < 3)
    def _():
        pl.semaphore_signal(barrier, inc=1, device_id=dev_up, device_id_type=MESH)

    @pl.when(z > 0)
    def _():
        pl.semaphore_signal(barrier, inc=1, device_id=dev_dn, device_id_type=MESH)

    edge = (z == 0) | (z == 3)

    @pl.when(edge)
    def _():
        pl.semaphore_wait(barrier, 5)

    @pl.when(jnp.logical_not(edge))
    def _():
        pl.semaphore_wait(barrier, 6)

    def rc(src, dst, ssem, rsem, dev):
        return pltpu.make_async_remote_copy(src_ref=src, dst_ref=dst, send_sem=ssem, recv_sem=rsem,
                                            device_id=dev, device_id_type=MESH)

    mine = pl.ds(pl.multiple_of(y * HALF, HALF), HALF)
    other = pl.ds(pl.multiple_of((1 - y) * HALF, HALF), HALF)

    def t_xx(b):
        return rc(xg.at[b], xg.at[b], x_xs, x_xr, dev_x)

    def t_xd(b):
        return rc(xg.at[b], xg.at[b], x_ds.at[b], x_dr.at[b], dev_s)

    def t_xu(b):
        return rc(xg.at[b], xg.at[b], x_us.at[b], x_ur.at[b], dev_up)

    def t_xn(b):
        return rc(xg.at[b], xg.at[b], x_ns.at[b], x_nr.at[b], dev_dn)

    def t_c(b):
        return rc(cp.at[b, other], crv.at[b], cs.at[b], cr.at[b], dev_y)

    def t_hy(b, rows):
        return rc(hg.at[b, cx, rows], hg.at[b, cx, rows], hys.at[b], hyr.at[b], dev_y)

    def t_hx(b, c, rows):
        return rc(hg.at[b, c, rows], hg.at[b, c, rows], hxs.at[b], hxr.at[b], dev_x)

    def t_gx(b, c, rows):
        return rc(hg.at[b, c, rows], hg.at[b, c, rows], gxs.at[b], gxr.at[b], dev_x)

    def t_d0(b, c):
        return rc(hg.at[b, c], hg.at[b, c], d0s.at[b], d0r.at[b], dev_s)

    def t_d1(b, c):
        return rc(hg.at[b, c], hg.at[b, c], d1s.at[b], d1r.at[b], dev_s)

    def t_zu(b):
        return rc(zp.at[b], zu.at[b], zs.at[b], zur.at[b], dev_up)

    def t_zn(b):
        return rc(zp.at[b], zd.at[b], zs.at[b], znr.at[b], dev_dn)

    low = 1 - z // 2

    def plane(s):
        return jnp.where(s == 0, z, jnp.where(s == 1, 1 + low, jnp.where(s == 2, 3 * low, z + 1 - 2 * (z % 2))))

    def xor(a, b):
        return ((a // 2 + b // 2) % 2) * 2 + (a + b) % 2

    def block(n, me):
        s, j = n // 4, n % 4
        return plane(s) * 4 + jnp.where(s < 2, xor(me, j), j)

    def when(cond):
        return pl.when(cond)

    loads[0].wait()
    own = z * 4 + cx
    far = z * 4 + xp
    t_xx(own).start()
    t_xd(own).start()

    @when(z < 3)
    def _():
        t_xu(own).start()

    @when(z > 0)
    def _():
        t_xn(own).start()

    def x_from_partner():
        t_xx(far).wait_recv()
        t_xd(far).start()

        @when(z < 2)
        def _():
            t_xu(far).start()

        @when(z > 1)
        def _():
            t_xn(far).start()

    def x_late():
        @when(z == 2)
        def _():
            t_xu(far).start()

        @when(z == 1)
        def _():
            t_xn(far).start()

    def x_hop(dist, c):
        @when(z >= dist)
        def _():
            b = (z - dist) * 4 + c
            t_xu(b).wait_recv()
            t_xd(b).start()

            @when(z < 3)
            def _():
                t_xu(b).start()

        @when(z + dist < 4)
        def _():
            b = (z + dist) * 4 + c
            t_xn(b).wait_recv()
            t_xd(b).start()

            @when(z > 0)
            def _():
                t_xn(b).start()

    def first_matmul(n):
        b = block(n, cx)

        @when((b + cx) % 2 == 1)
        def _():
            t_xd(b).wait_recv()

        cp[b] = jnp.dot(xg[b], w1[...], preferred_element_type=jnp.float32)
        t_c(b).start()

    def activation(n):
        b = block(n, cx)
        t_c(b).wait_recv()
        c = (cp[b, mine] + crv[b]).astype(jnp.bfloat16).astype(jnp.float32)
        t = jnp.tanh(math.sqrt(2 / math.pi) * (c + 0.044715 * (c * c * c)))
        hg[b, cx, mine] = (0.5 * c * (1.0 + t)).astype(jnp.bfloat16)
        t_hy(b, mine).start()
        t_hx(b, cx, mine).start()

    def pass_on_y(n):
        b = block(n, cx)
        t_hy(b, other).wait_recv()
        t_gx(b, cx, other).start()
        t_d0(b, cx).start()

    def pass_on_x(n):
        b = block(n, xp)
        t_hx(b, xp, mine).wait_recv()
        t_gx(b, xp, other).wait_recv()
        t_d1(b, xp).start()

    def second_matmul(b):
        t_d0(b, sib).wait_recv()
        t_d1(b, sibxp).wait_recv()
        acc = jnp.dot(hg[b, 0], w2[pl.ds(0, width)], preferred_element_type=jnp.float32)
        for c in range(1, 4):
            acc += jnp.dot(hg[b, c], w2[pl.ds(c * width, width)], preferred_element_type=jnp.float32)
        zp[b] = acc

    def z_send(b):
        @when(b // 4 > z)
        def _():
            t_zu(b).start()

        @when(b // 4 < z)
        def _():
            t_zn(b).start()

    def z_add(b):
        @when(b // 4 > z)
        def _():
            t_zu(b).wait_recv()
            zp[b] += zu[b]

        @when(b // 4 < z)
        def _():
            t_zn(b).wait_recv()
            zp[b] += zd[b]

        z_send(b)

    def finish(q):
        b = z * 4 + q

        @when(z > 0)
        def _():
            t_zu(b).wait_recv()
            zp[b] += zu[b]

        @when(z < 3)
        def _():
            t_zn(b).wait_recv()
            zp[b] += zd[b]

        @when(q == cx)
        def _():
            ab[q] = zp[b].astype(jnp.bfloat16)

        @when(q != cx)
        def _():
            fb[q] = zp[b].astype(jnp.bfloat16)
            rc(fb.at[q], ab.at[cx], a_s.at[q], a_r.at[cx], (z, y, q)).start()

    loads[1].wait()
    loads[2].wait()

    def step(i, carry):
        t = i - LEAD

        @when((t >= 0) & (t < BLOCKS))
        def _():
            activation(t)

        @when((t >= 1) & (t < BLOCKS + 1))
        def _():
            pass_on_y(t - 1)

        @when((t >= 2) & (t < BLOCKS + 2))
        def _():
            pass_on_x(t - 2)

        @when(t == 0)
        def _():
            x_from_partner()
            x_hop(1, cx)

        @when(t == 2)
        def _():
            x_hop(1, xp)
            x_hop(2, cx)

        @when(t == 4)
        def _():
            x_hop(2, xp)

        @when(t == 6)
        def _():
            x_hop(3, cx)
            x_hop(3, xp)

        @when(t == 7)
        def _():
            x_late()

        @when(t + LEAD < BLOCKS)
        def _():
            first_matmul(t + LEAD)

        n = t - 3
        group = (n == 3) | (n == 7)
        begin = jnp.where(group, n - 3, n)
        end = jnp.where((n > 7) | group, n + 1, begin)
        end = jnp.where(n < BLOCKS, end, begin)

        def one(m, carry):
            b = block(m, cx)
            second_matmul(b)

            @when(edge & (m > 3))
            def _():
                z_send(b)

            return carry

        lax.fori_loop(begin, end, one, 0)

        inner = jnp.logical_not(edge)

        @when(inner & (t >= 12) & (t < 16))
        def _():
            z_add(block(t - 8, cx))
            z_add(block(t - 4, cx))

        @when(inner & (n >= 12) & (n < 16))
        def _():
            z_add(block(n, cx))

        @when(t >= 16)
        def _():
            finish(t - 16)

        return carry

    lax.fori_loop(0, BLOCKS + 4 + LEAD, step, 0)

    def collect(c, carry):
        @when(c != cx)
        def _():
            rc(fb.at[c], ab.at[c], a_s.at[c], a_r.at[c], (z, y, c)).wait()

        return carry

    lax.fori_loop(0, 4, collect, 0)
    for c in range(4):
        out_ref[:, c * ab.shape[2]:(c + 1) * ab.shape[2]] = ab[c]

    def drain(b, carry):
        t_c(b).wait_send()
        t_hy(b, mine).wait_send()
        t_hx(b, cx, mine).wait_send()
        t_gx(b, cx, other).wait_send()
        t_d0(b, cx).wait_send()
        t_d1(b, xp).wait_send()
        p = b // 4

        @when(p != z)
        def _():
            t_zu(b).wait_send()

        @when((b + cx) % 2 == 0)
        def _():
            t_xd(b).wait_send()

            @when((z < 3) & (p <= z))
            def _():
                t_xu(b).wait_send()

            @when((z > 0) & (p >= z))
            def _():
                t_xn(b).wait_send()

        return carry

    lax.fori_loop(0, BLOCKS, drain, 0)
    t_xx(own).wait_send()


def solution(mesh):
    def body(x, w1, w2):
        dma = pltpu.SemaphoreType.DMA
        bf, f32 = jnp.bfloat16, jnp.float32
        depth, width = w1.shape
        cols = w2.shape[1]
        return pl.pallas_call(
            kernel,
            out_shape=jax.ShapeDtypeStruct(x.shape, bf),
            in_specs=[pl.BlockSpec(memory_space=pl.ANY)] * 3,
            out_specs=pl.BlockSpec(memory_space=pltpu.VMEM),
            scratch_shapes=[
                pltpu.VMEM((BLOCKS, ROWS, depth), bf),
                pltpu.VMEM(w1.shape, bf),
                pltpu.VMEM(w2.shape, bf),
                pltpu.VMEM((BLOCKS, ROWS, width), f32),
                pltpu.VMEM((BLOCKS, HALF, width), f32),
                pltpu.VMEM((BLOCKS, 4, ROWS, width), bf),
                pltpu.VMEM((BLOCKS, ROWS, cols), f32),
                pltpu.VMEM((BLOCKS, ROWS, cols), f32),
                pltpu.VMEM((BLOCKS, ROWS, cols), f32),
                pltpu.VMEM((4, ROWS, cols), bf),
                pltpu.VMEM((4, ROWS, cols), bf),
                dma((3,)), dma, dma,
            ] + [dma((BLOCKS,))] * 21 + [dma((4,)), dma((4,))],
            compiler_params=pltpu.CompilerParams(
                collective_id=0, has_side_effects=True, vmem_limit_bytes=56 * 2**20),
        )(x, w1, w2)

    return jax.shard_map(
        body,
        mesh=mesh,
        in_specs=(P(("cx", "cz"), "cy"), P("cy", ("cz", "cx")), P("cz", ("cy", "cx"))),
        out_specs=P(("cx", "cz"), "cy"),
        check_vma=False,
    )
```

```python
import math

import jax
import jax.numpy as jnp
from jax import lax
from jax.experimental import pallas as pl
from jax.experimental.pallas import tpu as pltpu
from jax.sharding import PartitionSpec as P

MESH = pl.DeviceIdType.MESH
ROWS = 64
HALF = ROWS // 2
BLOCKS = 16


def kernel(x_hbm, w1_hbm, w2_hbm, out_ref, xg, w1, w2, cp, crv, hg, zp, zu, zd, fb, ab, ld,
           sent, xr, cr, hyr, hxr, dr, zr, ar):
    z, y, cx = lax.axis_index("cz"), lax.axis_index("cy"), lax.axis_index("cx")
    core = cx % 2
    xp = (cx + 2) % 4
    sib = cx + 1 - 2 * core
    sibxp = (sib + 2) % 4
    dev_y = (z, 1 - y, cx)
    dev_x = (z, y, xp)
    dev_s = (z, y, sib)
    dev_up = ((z + 1) % 4, y, cx)
    dev_dn = ((z + 3) % 4, y, cx)
    width = w1.shape[1]
    slot, slot_xp = core * 2 + cx // 2, core * 2 + 1 - cx // 2
    pair_sib = pl.ds((1 - core) * 2, 2)

    loads = [pltpu.make_async_copy(x_hbm, xg.at[z * 4 + cx], ld.at[0]),
             pltpu.make_async_copy(w1_hbm, w1, ld.at[1]),
             pltpu.make_async_copy(w2_hbm, w2, ld.at[2])]
    for load in loads:
        load.start()

    barrier = pltpu.get_barrier_semaphore()
    for dev in (dev_y, dev_x, dev_s, (z, y, sibxp)):
        pl.semaphore_signal(barrier, inc=1, device_id=dev, device_id_type=MESH)

    @pl.when(z < 3)
    def _():
        pl.semaphore_signal(barrier, inc=1, device_id=dev_up, device_id_type=MESH)

    @pl.when(z > 0)
    def _():
        pl.semaphore_signal(barrier, inc=1, device_id=dev_dn, device_id_type=MESH)

    edge = (z == 0) | (z == 3)

    inner = jnp.logical_not(edge)

    @pl.when(edge)
    def _():
        pl.semaphore_wait(barrier, 5)

    @pl.when(inner)
    def _():
        pl.semaphore_wait(barrier, 6)

    def rc(src, dst, ssem, rsem, dev):
        return pltpu.make_async_remote_copy(src_ref=src, dst_ref=dst, send_sem=ssem, recv_sem=rsem,
                                            device_id=dev, device_id_type=MESH)

    mine = pl.ds(pl.multiple_of(y * HALF, HALF), HALF)
    other = pl.ds(pl.multiple_of((1 - y) * HALF, HALF), HALF)

    def t_xx(b):
        return rc(xg.at[b], xg.at[b], sent.at[0], xr.at[b], dev_x)

    def t_xd(b):
        return rc(xg.at[b], xg.at[b], sent.at[1], xr.at[b], dev_s)

    def t_xu(b):
        return rc(xg.at[b], xg.at[b], sent.at[2], xr.at[b], dev_up)

    def t_xn(b):
        return rc(xg.at[b], xg.at[b], sent.at[3], xr.at[b], dev_dn)

    def t_c(b):
        return rc(cp.at[b, other], crv.at[b], sent.at[4], cr.at[b], dev_y)

    def t_hy(b, rows):
        return rc(hg.at[b, slot, rows], hg.at[b, slot, rows], sent.at[5], hyr.at[b], dev_y)

    def t_hx(b, rows):
        return rc(hg.at[b, slot, rows], hg.at[b, slot, rows], sent.at[6], hxr.at[b], dev_x)

    def t_hd(b, c):
        return rc(hg.at[b, c], hg.at[b, c], sent.at[7], dr.at[b], dev_s)

    def t_zu(b):
        return rc(zp.at[b], zu.at[b], sent.at[8], zr.at[b], dev_up)

    def t_zn(b, last):
        return rc(zp.at[b], zd.at[b], sent.at[8], zr.at[jnp.where(last, BLOCKS + b % 4, b)], dev_dn)

    def t_a(q, frm):
        return rc(fb.at[q], ab.at[frm], sent.at[9], ar.at[frm], (z, y, q))

    low = 1 - z // 2

    def plane(s):
        return jnp.where(s == 0, z, jnp.where(s == 1, 1 + low, jnp.where(s == 2, 3 * low, z + 1 - 2 * (z % 2))))

    def xor(a, b):
        return ((a // 2 + b // 2) % 2) * 2 + (a + b) % 2

    def block(n, me):
        s, j = n // 4, n % 4
        return plane(s) * 4 + jnp.where(s < 2, xor(me, j), j)

    def when(cond):
        return pl.when(cond)

    loads[0].wait()
    own = z * 4 + cx
    far = z * 4 + xp
    t_xx(own).start()
    t_xd(own).start()

    @when(z < 3)
    def _():
        t_xu(own).start()

    @when(z > 0)
    def _():
        t_xn(own).start()

    def x_from_partner():
        t_xx(far).wait_recv()
        t_xd(far).start()

        @when(z < 2)
        def _():
            t_xu(far).start()

        @when(z > 1)
        def _():
            t_xn(far).start()

    def x_late():
        @when(z == 2)
        def _():
            t_xu(far).start()

        @when(z == 1)
        def _():
            t_xn(far).start()

    def x_hop(dist, c, where=True):
        @when((z >= dist) & where)
        def _():
            b = (z - dist) * 4 + c
            t_xu(b).wait_recv()
            t_xd(b).start()

            @when(z < 3)
            def _():
                t_xu(b).start()

        @when((z + dist < 4) & where)
        def _():
            b = (z + dist) * 4 + c
            t_xn(b).wait_recv()
            t_xd(b).start()

            @when(z > 0)
            def _():
                t_xn(b).start()

    def first_matmul(n):
        b = block(n, cx)

        @when((b + cx) % 2 == 1)
        def _():
            t_xd(b).wait_recv()

        cp[b] = jnp.dot(xg[b], w1[...], preferred_element_type=jnp.float32)
        t_c(b).start()

    def activation(n):
        b = block(n, cx)
        t_c(b).wait_recv()
        c = (cp[b, mine] + crv[b]).astype(jnp.bfloat16).astype(jnp.float32)
        t = jnp.tanh(math.sqrt(2 / math.pi) * (c + 0.044715 * (c * c * c)))
        hg[b, slot, mine] = (0.5 * c * (1.0 + t)).astype(jnp.bfloat16)
        t_hy(b, mine).start()
        t_hx(b, mine).start()

    def pass_on_y(n):
        b = block(n, cx)
        t_hy(b, other).wait_recv()
        t_hx(b, other).start()
        t_hd(b, slot).start()

    def pass_on_x(n):
        b = block(n, xp)
        piece = hg.at[b, slot_xp]
        rc(piece, piece, sent.at[6], hxr.at[b], dev_x).wait_recv()
        t_hd(b, slot_xp).start()

    def second_matmul(b):
        pieces = hg.at[b, pair_sib]
        rc(pieces, pieces, sent.at[7], dr.at[b], dev_s).wait_recv()
        acc = jnp.dot(hg[b, 0], w2[pl.ds(0, width)], preferred_element_type=jnp.float32)
        for i in range(1, 4):
            c = (i % 2) * 2 + i // 2
            acc += jnp.dot(hg[b, i], w2[pl.ds(c * width, width)], preferred_element_type=jnp.float32)
        zp[b] = acc

    def z_send(b):
        @when(b // 4 > z)
        def _():
            t_zu(b).start()

        @when(b // 4 < z)
        def _():
            t_zn(b, b // 4 == z - 1).start()

    def z_add(b):
        @when(b // 4 > z)
        def _():
            t_zu(b).wait_recv()
            zp[b] += zu[b]

        @when(b // 4 < z)
        def _():
            t_zn(b, False).wait_recv()
            zp[b] += zd[b]

        z_send(b)

    def finish(q):
        b = z * 4 + q

        @when(z > 0)
        def _():
            t_zu(b).wait_recv()
            zp[b] += zu[b]

        @when(z < 3)
        def _():
            t_zn(b, True).wait_recv()
            zp[b] += zd[b]

        @when(q == cx)
        def _():
            ab[q] = zp[b].astype(jnp.bfloat16)

        @when(q != cx)
        def _():
            fb[q] = zp[b].astype(jnp.bfloat16)
            t_a(q, cx).start()

    loads[1].wait()

    def lead(t):
        return jnp.minimum(BLOCKS, t + 2 + jnp.clip(t - 12, 0, 1))

    def partial_c(n, carry):
        first_matmul(n)
        return carry

    def partial_z(b):
        second_matmul(b)

        @when(edge & (b // 4 != z))
        def _():
            z_send(b)

    away = plane(1) * 4

    def step(i, carry):
        t = i - 2

        @when((t >= 0) & (t < BLOCKS))
        def _():
            activation(t)

        @when(t == 0)
        def _():
            x_from_partner()
            x_hop(1, cx)

        @when(t == 2)
        def _():
            x_hop(1, xp, inner)
            x_hop(2, cx, edge)

        @when(t == 3)
        def _():
            x_hop(2, cx, inner)

        @when(t == 4)
        def _():
            x_hop(2, xp)

        @when(t == 6)
        def _():
            x_hop(3, cx)
            x_hop(3, xp)

        @when(t == 7)
        def _():
            x_late()

        @when(t == 9)
        def _():
            x_hop(1, xp, edge)

        lax.fori_loop(jnp.where(t == -2, 0, lead(t)), lead(t + 1), partial_c, 0)

        @when(t == 5)
        def _():
            loads[2].wait()

        one = (t >= 6) & (t < 19)
        two = (t == 10) | (t == 12) | (t == 14)

        def partial(m, carry):
            own_b = z * 4 + t - 6
            far_b = away + jnp.where(t == 10, m, t // 2 - 4)
            late_b = block(t - 3, cx)
            partial_z(jnp.where(t < 10, own_b, jnp.where((t == 10) | (m == 1), far_b, late_b)))
            return carry

        lax.fori_loop(0, jnp.where(two, 2, jnp.where(one, 1, 0)), partial, 0)

        @when(inner & (t >= 15) & (t < 19))
        def _():
            z_add(block(t - 3, cx))

        @when((t >= 1) & (t < BLOCKS + 1))
        def _():
            pass_on_y(t - 1)

        @when((t >= 2) & (t < BLOCKS + 2))
        def _():
            pass_on_x(t - 2)

        @when(inner & (t == 12))
        def _():
            z_add(away)
            z_add(away + 1)

        @when(inner & ((t == 14) | (t == 16)))
        def _():
            z_add(away + t // 2 - 5)

        @when(inner & ((t == 13) | (t == 14)))
        def _():
            z_add(block(t - 5, cx))

        @when(inner & ((t == 14) | (t == 15)))
        def _():
            z_add(block(t - 4, cx))

        @when(t >= 18)
        def _():
            finish(t - 18)

        return carry

    lax.fori_loop(0, BLOCKS + 8, step, 0)

    def collect(c, carry):
        @when(c != cx)
        def _():
            t_a(c, c).wait_recv()

        return carry

    lax.fori_loop(0, 4, collect, 0)
    def gather_out():
        for c in range(4):
            out_ref[:, c * ab.shape[2]:(c + 1) * ab.shape[2]] = ab[c]

    gather_out()

    def sent_all(kind, ref, dev):
        rc(ref, ref, sent.at[kind], xr.at[0], dev).wait_send()

    def wait_sends():
        sent_all(0, xg.at[own], dev_x)
        sent_all(1, xg.at[pl.ds(0, 8)], dev_s)
        for k in range(4):
            @when(z == k)
            def _(k=k):
                if k < 3:
                    sent_all(2, xg.at[pl.ds(0, 2 * (k + 1))], dev_up)
                if k > 0:
                    sent_all(3, xg.at[pl.ds(0, 2 * (4 - k))], dev_dn)
        sent_all(4, crv, dev_y)
        sent_all(5, hg.at[pl.ds(0, 2)], dev_y)
        sent_all(6, hg.at[pl.ds(0, 4)], dev_x)
        sent_all(7, hg.at[pl.ds(0, 8)], dev_s)
        sent_all(8, zp.at[pl.ds(0, 12)], dev_y)
        sent_all(9, fb.at[pl.ds(0, 3)], dev_x)

    wait_sends()


def solution(mesh):
    def body(x, w1, w2):
        dma = pltpu.SemaphoreType.DMA
        bf, f32 = jnp.bfloat16, jnp.float32
        depth, width = w1.shape
        cols = w2.shape[1]
        return pl.pallas_call(
            kernel,
            out_shape=jax.ShapeDtypeStruct(x.shape, bf),
            in_specs=[pl.BlockSpec(memory_space=pltpu.HBM)] * 3,
            out_specs=pl.BlockSpec(memory_space=pltpu.VMEM),
            scratch_shapes=[
                pltpu.VMEM((BLOCKS, ROWS, depth), bf),
                pltpu.VMEM(w1.shape, bf),
                pltpu.VMEM(w2.shape, bf),
                pltpu.VMEM((BLOCKS, ROWS, width), f32),
                pltpu.VMEM((BLOCKS, HALF, width), f32),
                pltpu.VMEM((BLOCKS, 4, ROWS, width), bf),
                pltpu.VMEM((BLOCKS, ROWS, cols), f32),
                pltpu.VMEM((BLOCKS, ROWS, cols), f32),
                pltpu.VMEM((BLOCKS, ROWS, cols), f32),
                pltpu.VMEM((4, ROWS, cols), bf),
                pltpu.VMEM((4, ROWS, cols), bf),
                dma((3,)), dma((10,)),
            ] + [dma((BLOCKS,))] * 5 + [dma((BLOCKS + 4,)), dma((4,))],
            compiler_params=pltpu.CompilerParams(
                collective_id=0, has_side_effects=True, vmem_limit_bytes=56_150_000),
        )(x, w1, w2)

    return jax.shard_map(
        body,
        mesh=mesh,
        in_specs=(P(("cx", "cz"), "cy"), P("cy", ("cz", "cx")), P("cz", ("cy", "cx"))),
        out_specs=P(("cx", "cz"), "cy"),
        check_vma=False,
    )
```

```python
import math

import jax
import jax.numpy as jnp
from jax import lax
from jax.experimental import pallas as pl
from jax.experimental.pallas import tpu as pltpu
from jax.sharding import PartitionSpec as P

MESH = pl.DeviceIdType.MESH
ROWS = 64
HALF = ROWS // 2
BLOCKS = 16


def kernel(x_hbm, w1_hbm, w2_hbm, out_ref, xg, w1, w2, cp, crv, hg, zp, zu, zd, fb, ab, ld,
           sent, xr, cr, hyr, hxr, dr, zr, ar):
    z, y, cx = lax.axis_index("cz"), lax.axis_index("cy"), lax.axis_index("cx")
    core = cx % 2
    xp = (cx + 2) % 4
    sib = cx + 1 - 2 * core
    dev_y = (z, 1 - y, cx)
    dev_x = (z, y, xp)
    dev_s = (z, y, sib)
    dev_up = ((z + 1) % 4, y, cx)
    dev_dn = ((z + 3) % 4, y, cx)
    width = w1.shape[1]
    left, right = pl.ds(0, width // 2), pl.ds(width // 2, width // 2)
    slot, slot_xp = core * 2 + cx // 2, core * 2 + 1 - cx // 2
    pair_sib = pl.ds((1 - core) * 2, 2)

    loads = [pltpu.make_async_copy(x_hbm, xg.at[z * 4 + cx], ld.at[0]),
             pltpu.make_async_copy(w1_hbm.at[:, left], w1.at[:, left], ld.at[1]),
             pltpu.make_async_copy(w1_hbm.at[:, right], w1.at[:, right], ld.at[2]),
             pltpu.make_async_copy(w2_hbm, w2, ld.at[3])]
    for load in loads:
        load.start()

    barrier = pltpu.get_barrier_semaphore()
    near = z + 1 - 2 * (z % 2)
    for dev in (dev_y, dev_x, dev_s, (near, y, xp), (near, y, sib), (near, y, (sib + 2) % 4)):
        pl.semaphore_signal(barrier, inc=1, device_id=dev, device_id_type=MESH)

    @pl.when(z < 3)
    def _():
        pl.semaphore_signal(barrier, inc=1, device_id=dev_up, device_id_type=MESH)

    @pl.when(z > 0)
    def _():
        pl.semaphore_signal(barrier, inc=1, device_id=dev_dn, device_id_type=MESH)

    edge = (z == 0) | (z == 3)

    inner = jnp.logical_not(edge)

    @pl.when(edge)
    def _():
        pl.semaphore_wait(barrier, 7)

    @pl.when(inner)
    def _():
        pl.semaphore_wait(barrier, 8)

    def rc(src, dst, ssem, rsem, dev):
        return pltpu.make_async_remote_copy(src_ref=src, dst_ref=dst, send_sem=ssem, recv_sem=rsem,
                                            device_id=dev, device_id_type=MESH)

    mine = pl.ds(pl.multiple_of(y * HALF, HALF), HALF)
    other = pl.ds(pl.multiple_of((1 - y) * HALF, HALF), HALF)

    def t_xx(b):
        return rc(xg.at[b], xg.at[b], sent.at[0], xr.at[b], dev_x)

    def t_xd(b):
        return rc(xg.at[b], xg.at[b], sent.at[1], xr.at[b], dev_s)

    def t_xu(b):
        return rc(xg.at[b], xg.at[b], sent.at[2], xr.at[b], dev_up)

    def t_xn(b):
        return rc(xg.at[b], xg.at[b], sent.at[3], xr.at[b], dev_dn)

    def t_c(b):
        return rc(cp.at[b, other], crv.at[b], sent.at[4], cr.at[b], dev_y)

    def t_hy(b, rows):
        return rc(hg.at[b, slot, rows], hg.at[b, slot, rows], sent.at[5], hyr.at[b], dev_y)

    def t_hx(b, rows):
        return rc(hg.at[b, slot, rows], hg.at[b, slot, rows], sent.at[6], hxr.at[b], dev_x)

    def t_hd(b, c):
        return rc(hg.at[b, c], hg.at[b, c], sent.at[7], dr.at[b], dev_s)

    def t_zu(b):
        return rc(zp.at[b], zu.at[b], sent.at[8], zr.at[b], dev_up)

    def t_zn(b, last):
        return rc(zp.at[b], zd.at[b], sent.at[8], zr.at[jnp.where(last, BLOCKS + b % 4, b)], dev_dn)

    def t_a(q, frm):
        return rc(fb.at[q], ab.at[frm], sent.at[9], ar.at[frm], (near, y, q))

    low = 1 - z // 2

    def plane(s):
        return jnp.where(s == 0, z, jnp.where(s == 1, 1 + low, jnp.where(s == 2, 3 * low, near)))

    def xor(a, b):
        return ((a // 2 + b // 2) % 2) * 2 + (a + b) % 2

    def block(n, me):
        s, j = n // 4, n % 4
        return plane(s) * 4 + jnp.where(s == 0, xor(me, j), jnp.where(s == 1, (me // 2 * 2 + j) % 4, j))

    def when(cond):
        return pl.when(cond)

    loads[0].wait()
    own = z * 4 + cx
    far = z * 4 + xp
    t_xx(own).start()
    t_xd(own).start()

    @when(z < 3)
    def _():
        t_xu(own).start()

    @when(z > 0)
    def _():
        t_xn(own).start()

    def x_from_partner():
        t_xx(far).wait_recv()
        t_xd(far).start()

        @when(z < 2)
        def _():
            t_xu(far).start()

        @when(z > 1)
        def _():
            t_xn(far).start()

    def x_late():
        @when(z == 2)
        def _():
            t_xu(far).start()

        @when(z == 1)
        def _():
            t_xn(far).start()

    def x_hop(dist, c, where=True):
        @when((z >= dist) & where)
        def _():
            b = (z - dist) * 4 + c
            t_xu(b).wait_recv()
            t_xd(b).start()

            @when(z < 3)
            def _():
                t_xu(b).start()

        @when((z + dist < 4) & where)
        def _():
            b = (z + dist) * 4 + c
            t_xn(b).wait_recv()
            t_xd(b).start()

            @when(z > 0)
            def _():
                t_xn(b).start()

    def first_matmul(n):
        b = block(n, cx)

        @when((b + cx) % 2 == 1)
        def _():
            t_xd(b).wait_recv()

        cp[b] = jnp.dot(xg[b], w1[...], preferred_element_type=jnp.float32)
        t_c(b).start()

    def activation(n):
        b = block(n, cx)
        t_c(b).wait_recv()
        c = (cp[b, mine] + crv[b]).astype(jnp.bfloat16).astype(jnp.float32)
        t = jnp.tanh(math.sqrt(2 / math.pi) * (c + 0.044715 * (c * c * c)))
        hg[b, slot, mine] = (0.5 * c * (1.0 + t)).astype(jnp.bfloat16)
        t_hy(b, mine).start()
        t_hx(b, mine).start()

    def pass_on_y(n):
        b = block(n, cx)
        t_hy(b, other).wait_recv()
        t_hx(b, other).start()
        t_hd(b, slot).start()

    def pass_on_x(n):
        b = block(n, xp)
        piece = hg.at[b, slot_xp]
        rc(piece, piece, sent.at[6], hxr.at[b], dev_x).wait_recv()
        t_hd(b, slot_xp).start()

    def second_matmul(b):
        pieces = hg.at[b, pair_sib]
        rc(pieces, pieces, sent.at[7], dr.at[b], dev_s).wait_recv()
        acc = jnp.dot(hg[b, 0], w2[pl.ds(0, width)], preferred_element_type=jnp.float32)
        for i in range(1, 4):
            c = (i % 2) * 2 + i // 2
            acc += jnp.dot(hg[b, i], w2[pl.ds(c * width, width)], preferred_element_type=jnp.float32)
        zp[b] = acc

    def last_plane(b):
        p = b // 4
        return p + 1 - 2 * (p % 2)

    def z_send(b):
        @when(last_plane(b) > z)
        def _():
            t_zu(b).start()

        @when(last_plane(b) < z)
        def _():
            t_zn(b, last_plane(b) == z - 1).start()

    def z_add(b):
        @when(last_plane(b) > z)
        def _():
            t_zu(b).wait_recv()
            zp[b] += zu[b]

        @when(last_plane(b) < z)
        def _():
            t_zn(b, False).wait_recv()
            zp[b] += zd[b]

        z_send(b)

    def finish(q):
        b = near * 4 + q

        @when(z > 0)
        def _():
            t_zu(b).wait_recv()
            zp[b] += zu[b]

        @when(z < 3)
        def _():
            t_zn(b, True).wait_recv()
            zp[b] += zd[b]

        fb[q] = zp[b].astype(jnp.bfloat16)
        t_a(q, cx).start()

    for load, cols in ((loads[1], left), (loads[2], right)):
        load.wait()
        cp[own, :, cols] = jnp.dot(xg[own], w1[:, cols], preferred_element_type=jnp.float32)
        rc(cp.at[own, other, cols], crv.at[own, :, cols], sent.at[4], cr.at[own], dev_y).start()

    def lead(t):
        return jnp.minimum(BLOCKS, t + 2 + jnp.clip(t - 11, 0, 1))

    def partial_c(n, carry):
        first_matmul(n)
        return carry

    def partial_z(b):
        second_matmul(b)

        @when(edge & (b // 4 != near))
        def _():
            z_send(b)

    away = plane(1) * 4

    def step(i, carry):
        t = i - 1

        @when(inner & (t == 11))
        def _():
            z_add(away)

        @when(t == 15)
        def _():
            pass_on_y(12)

        @when((t >= 0) & (t < BLOCKS))
        def _():
            activation(t)

        @when(t == 16)
        def _():
            pass_on_y(15)

        @when(inner & (t == 16))
        def _():
            z_add(block(11, cx))

        @when(t == 17)
        def _():
            pass_on_x(15)

        @when(t == 0)
        def _():
            x_from_partner()
            x_hop(1, cx)

        @when(t == 2)
        def _():
            x_hop(1, xp, inner)
            x_hop(2, cx, edge)

        @when(t == 3)
        def _():
            x_hop(2, cx, inner)

        @when(t == 4)
        def _():
            x_hop(2, xp)

        @when(t == 6)
        def _():
            x_hop(3, cx)
            x_hop(3, xp)

        @when(t == 7)
        def _():
            x_late()

        @when(t == 9)
        def _():
            x_hop(1, xp, edge)

        lax.fori_loop(lead(t), lead(t + 1), partial_c, 0)

        @when(t == 5)
        def _():
            loads[3].wait()

        def partial(m, carry):
            own_b = z * 4 + jnp.where(t == 6, m, t - 5)
            late = block(t - 3 - t // 16 + t // 17, cx)
            partial_z(jnp.where(t < 9, own_b, jnp.where(t < 11, away + t - 9 + 2 * m, late)))
            return carry

        two = (t == 6) | (t == 9) | (t == 10)
        lax.fori_loop(0, jnp.where(two, 2, jnp.where((t >= 6) & (t != 15), 1, 0)), partial, 0)

        @when(t == 16)
        def _():
            finish(0)
            pass_on_x(13)
            pass_on_x(14)
            partial_z(block(13, cx))

        @when(inner & (t == 12))
        def _():
            z_add(away + 1)

        @when((t >= 1) & (t < 13))
        def _():
            pass_on_y(t - 1)

        @when((t >= 2) & (t < 14))
        def _():
            pass_on_x(t - 2)

        @when(t == 15)
        def _():
            pass_on_y(13)
            pass_on_y(14)

        @when(inner & ((t == 11) | (t == 12)))
        def _():
            z_add(away + t - 9)

        @when(inner & (t >= 13) & (t < 16))
        def _():
            z_add(block(t - 5, cx))

        @when(inner & (t == 13))
        def _():
            z_add(z * 4)
            z_add(z * 4 + 2)

        @when(inner & ((t == 14) | (t == 15)))
        def _():
            z_add(z * 4 + 2 * t - 27)

        @when(t == 15)
        def _():
            pass_on_x(12)

        @when(t >= 16)
        def _():
            finish(t - 15)

        return carry

    lax.fori_loop(0, BLOCKS + 4, step, 0)

    def collect(c, carry):
        t_a(c, c).wait_recv()
        return carry

    lax.fori_loop(0, 4, collect, 0)
    def gather_out():
        for c in range(4):
            out_ref[:, c * ab.shape[2]:(c + 1) * ab.shape[2]] = ab[c]

    gather_out()

    def sent_all(kind, ref, dev):
        rc(ref, ref, sent.at[kind], xr.at[0], dev).wait_send()

    def wait_sends():
        sent_all(0, xg.at[own], dev_x)
        sent_all(1, xg.at[pl.ds(0, 8)], dev_s)
        for k in range(4):
            @when(z == k)
            def _(k=k):
                if k < 3:
                    sent_all(2, xg.at[pl.ds(0, 2 * (k + 1))], dev_up)
                if k > 0:
                    sent_all(3, xg.at[pl.ds(0, 2 * (4 - k))], dev_dn)
        sent_all(4, crv, dev_y)
        sent_all(5, hg.at[pl.ds(0, 2)], dev_y)
        sent_all(6, hg.at[pl.ds(0, 4)], dev_x)
        sent_all(7, hg.at[pl.ds(0, 8)], dev_s)
        sent_all(8, zp.at[pl.ds(0, 12)], dev_y)
        sent_all(9, fb, dev_x)

    wait_sends()


def solution(mesh):
    def body(x, w1, w2):
        dma = pltpu.SemaphoreType.DMA
        bf, f32 = jnp.bfloat16, jnp.float32
        depth, width = w1.shape
        cols = w2.shape[1]
        return pl.pallas_call(
            kernel,
            out_shape=jax.ShapeDtypeStruct(x.shape, bf),
            in_specs=[pl.BlockSpec(memory_space=pltpu.HBM)] * 3,
            out_specs=pl.BlockSpec(memory_space=pltpu.VMEM),
            scratch_shapes=[
                pltpu.VMEM((BLOCKS, ROWS, depth), bf),
                pltpu.VMEM(w1.shape, bf),
                pltpu.VMEM(w2.shape, bf),
                pltpu.VMEM((BLOCKS, ROWS, width), f32),
                pltpu.VMEM((BLOCKS, HALF, width), f32),
                pltpu.VMEM((BLOCKS, 4, ROWS, width), bf),
                pltpu.VMEM((BLOCKS, ROWS, cols), f32),
                pltpu.VMEM((BLOCKS, ROWS, cols), f32),
                pltpu.VMEM((BLOCKS, ROWS, cols), f32),
                pltpu.VMEM((4, ROWS, cols), bf),
                pltpu.VMEM((4, ROWS, cols), bf),
                dma((4,)), dma((10,)),
            ] + [dma((BLOCKS,))] * 5 + [dma((BLOCKS + 4,)), dma((4,))],
            compiler_params=pltpu.CompilerParams(
                collective_id=0, has_side_effects=True, vmem_limit_bytes=56_150_000),
        )(x, w1, w2)

    return jax.shard_map(
        body,
        mesh=mesh,
        in_specs=(P(("cx", "cz"), "cy"), P("cy", ("cz", "cx")), P("cz", ("cy", "cx"))),
        out_specs=P(("cx", "cz"), "cy"),
        check_vma=False,
    )
```

```python
import math

import jax
import jax.numpy as jnp
from jax import lax
from jax.experimental import pallas as pl
from jax.experimental.pallas import tpu as pltpu
from jax.sharding import PartitionSpec as P

MESH = pl.DeviceIdType.MESH
ROWS = 64
HALF = ROWS // 2
BLOCKS = 16


def kernel(x_hbm, w1_hbm, w2_hbm, out_ref, xg, w1, w2, cp, crv, hg, zp, zu, zd, fb, ab, ld,
           sent, xr, cr, hyr, hxr, dr, zr, ar):
    z, y, cx = lax.axis_index("cz"), lax.axis_index("cy"), lax.axis_index("cx")
    core = cx % 2
    xp = (cx + 2) % 4
    sib = cx + 1 - 2 * core
    dev_y = (z, 1 - y, cx)
    dev_x = (z, y, xp)
    dev_s = (z, y, sib)
    dev_up = ((z + 1) % 4, y, cx)
    dev_dn = ((z + 3) % 4, y, cx)
    width = w1.shape[1]
    left, right = pl.ds(0, width // 2), pl.ds(width // 2, width // 2)
    slot, slot_xp = core * 2 + cx // 2, core * 2 + 1 - cx // 2
    pair_sib = pl.ds((1 - core) * 2, 2)

    loads = [pltpu.make_async_copy(x_hbm, xg.at[z * 4 + cx], ld.at[0]),
             pltpu.make_async_copy(w1_hbm.at[:, left], w1.at[:, left], ld.at[1]),
             pltpu.make_async_copy(w1_hbm.at[:, right], w1.at[:, right], ld.at[2])]
    for load in loads:
        load.start()

    barrier = pltpu.get_barrier_semaphore()
    near = z + 1 - 2 * (z % 2)
    for dev in (dev_y, dev_x, dev_s, (near, y, xp), (near, y, sib), (near, y, (sib + 2) % 4)):
        pl.semaphore_signal(barrier, inc=1, device_id=dev, device_id_type=MESH)

    @pl.when(z < 3)
    def _():
        pl.semaphore_signal(barrier, inc=1, device_id=dev_up, device_id_type=MESH)

    @pl.when(z > 0)
    def _():
        pl.semaphore_signal(barrier, inc=1, device_id=dev_dn, device_id_type=MESH)

    edge = (z == 0) | (z == 3)

    inner = jnp.logical_not(edge)

    @pl.when(edge)
    def _():
        pl.semaphore_wait(barrier, 7)

    @pl.when(inner)
    def _():
        pl.semaphore_wait(barrier, 8)

    def rc(src, dst, ssem, rsem, dev):
        return pltpu.make_async_remote_copy(src_ref=src, dst_ref=dst, send_sem=ssem, recv_sem=rsem,
                                            device_id=dev, device_id_type=MESH)

    mine = pl.ds(pl.multiple_of(y * HALF, HALF), HALF)
    other = pl.ds(pl.multiple_of((1 - y) * HALF, HALF), HALF)

    def turn(b):
        p = b // 4
        return b % 4 + jnp.where((p == near) | (p == 2 - z // 2), 4, 0)

    def t_xx(b):
        return rc(xg.at[b], xg.at[b], sent.at[0], xr.at[b], dev_x)

    def t_xd(b):
        return rc(xg.at[b], xg.at[b], sent.at[1], xr.at[b], dev_s)

    def t_xu(b):
        return rc(xg.at[b], xg.at[b], sent.at[2], xr.at[b], dev_up)

    def t_xn(b):
        return rc(xg.at[b], xg.at[b], sent.at[3], xr.at[b], dev_dn)

    def t_c(b):
        return rc(cp.at[b, other], crv.at[b], sent.at[4], cr.at[turn(b)], dev_y)

    def t_hy(b, rows):
        return rc(hg.at[b, slot, rows], hg.at[b, slot, rows], sent.at[5], hyr.at[turn(b)], dev_y)

    def t_hx(b, rows):
        return rc(hg.at[b, slot, rows], hg.at[b, slot, rows], sent.at[6], hxr.at[turn(b)], dev_x)

    def t_hd(b, c):
        return rc(hg.at[b, c], hg.at[b, c], sent.at[7], dr.at[turn(b)], dev_s)

    def t_zu(b):
        return rc(zp.at[b], zu.at[b], sent.at[8], zr.at[b], dev_up)

    def t_zn(b, last):
        return rc(zp.at[b], zd.at[b], sent.at[8], zr.at[jnp.where(last, BLOCKS + b % 4, b)], dev_dn)

    def t_a(q, frm):
        return rc(fb.at[q], ab.at[frm], sent.at[9], ar.at[frm], (near, y, q))

    low = 1 - z // 2

    def plane(s):
        return jnp.where(s == 0, z, jnp.where(s == 1, 1 + low, jnp.where(s == 2, 3 * low, near)))

    def block(n, me):
        s, j = n // 4, n % 4
        chip = me // 2 * 2
        own_first = chip + jnp.where(s == 1, j + 1 - 2 * (j % 2), jnp.where(j < 2, (me + j) % 2, j))
        return plane(s) * 4 + jnp.where(s < 2, own_first % 4, j)

    def when(cond):
        return pl.when(cond)

    loads[0].wait()
    own = z * 4 + cx
    far = z * 4 + xp
    t_xd(own).start()

    def x_line():
        @when(z < 3)
        def _():
            t_xu(own).start()

        @when(z > 0)
        def _():
            t_xn(own).start()

    @when(core == 0)
    def _():
        t_xx(own).start()

    @when(core == 1)
    def _():
        x_line()

    def x_from_partner():
        t_xx(far).wait_recv()
        t_xd(far).start()

        @when(z < 2)
        def _():
            t_xu(far).start()

        @when(z > 1)
        def _():
            t_xn(far).start()

    def x_late():
        @when(z == 2)
        def _():
            t_xu(far).start()

        @when(z == 1)
        def _():
            t_xn(far).start()

    def x_hop(dist, c, where=True):
        @when((z >= dist) & where)
        def _():
            b = (z - dist) * 4 + c
            t_xu(b).wait_recv()
            t_xd(b).start()

            @when(z < 3)
            def _():
                t_xu(b).start()

        @when((z + dist < 4) & where)
        def _():
            b = (z + dist) * 4 + c
            t_xn(b).wait_recv()
            t_xd(b).start()

            @when(z > 0)
            def _():
                t_xn(b).start()

    def first_matmul(n):
        b = block(n, cx)

        @when((b + cx) % 2 == 1)
        def _():
            t_xd(b).wait_recv()

        cp[b] = jnp.dot(xg[b], w1[...], preferred_element_type=jnp.float32)
        t_c(b).start()

    def activation(n):
        b = block(n, cx)
        t_c(b).wait_recv()
        c = (cp[b, mine] + crv[b]).astype(jnp.bfloat16).astype(jnp.float32)
        t = jnp.tanh(math.sqrt(2 / math.pi) * (c + 0.044715 * (c * c * c)))
        hg[b, slot, mine] = (0.5 * c * (1.0 + t)).astype(jnp.bfloat16)
        t_hy(b, mine).start()
        t_hx(b, mine).start()

    def pass_on_y(n):
        b = block(n, cx)
        t_hy(b, other).wait_recv()
        t_hx(b, other).start()
        t_hd(b, slot).start()

    def pass_on_x(n):
        b = block(n, xp)
        piece = hg.at[b, slot_xp]
        rc(piece, piece, sent.at[6], hxr.at[turn(b)], dev_x).wait_recv()
        t_hd(b, slot_xp).start()

    def second_matmul(b):
        pieces = hg.at[b, pair_sib]
        rc(pieces, pieces, sent.at[7], dr.at[turn(b)], dev_s).wait_recv()
        acc = jnp.dot(hg[b, 0], w2[pl.ds(0, width)], preferred_element_type=jnp.float32)
        for i in range(1, 4):
            c = (i % 2) * 2 + i // 2
            acc += jnp.dot(hg[b, i], w2[pl.ds(c * width, width)], preferred_element_type=jnp.float32)
        zp[b] = acc

    def last_plane(b):
        p = b // 4
        return p + 1 - 2 * (p % 2)

    def z_send(b):
        @when(last_plane(b) > z)
        def _():
            t_zu(b).start()

        @when(last_plane(b) < z)
        def _():
            t_zn(b, last_plane(b) == z - 1).start()

    def z_add(b):
        @when(last_plane(b) > z)
        def _():
            t_zu(b).wait_recv()
            zp[b] += zu[b]

        @when(last_plane(b) < z)
        def _():
            t_zn(b, False).wait_recv()
            zp[b] += zd[b]

        z_send(b)

    def finish(q):
        b = near * 4 + q

        @when(z > 0)
        def _():
            t_zu(b).wait_recv()
            zp[b] += zu[b]

        @when(z < 3)
        def _():
            t_zn(b, True).wait_recv()
            zp[b] += zd[b]

        fb[q] = zp[b].astype(jnp.bfloat16)
        t_a(q, cx).start()

    for load, cols in ((loads[1], left), (loads[2], right)):
        load.wait()
        cp[own, :, cols] = jnp.dot(xg[own], w1[:, cols], preferred_element_type=jnp.float32)
        rc(cp.at[own, other, cols], crv.at[own, :, cols], sent.at[4], cr.at[turn(own)], dev_y).start()

    @when(core == 0)
    def _():
        x_line()

    @when(core == 1)
    def _():
        t_xx(own).start()

    first_matmul(1)

    def lead(t):
        return jnp.minimum(BLOCKS, t + 2 + jnp.clip(t - 11, 0, 1) + jnp.where((t == 0) & (core == 0) | (t < 0), 1, 0))

    def partial_c(n, carry):
        first_matmul(n)
        return carry

    def partial_z(b):
        second_matmul(b)

        @when(edge & (b // 4 != near))
        def _():
            z_send(b)

    away = plane(1) * 4

    def step(i, carry):
        t = i - 1

        @when(inner & (t == 11))
        def _():
            z_add(away + 1)

        @when(t == 15)
        def _():
            pass_on_y(12)

        @when((t >= 0) & (t < BLOCKS))
        def _():
            activation(t)

        @when(t == 16)
        def _():
            pass_on_y(15)

        @when(t == 17)
        def _():
            pass_on_x(15)

        @when((t < 0) & (core == 0))
        def _():
            x_from_partner()

        @when((t < 0) & (core == 1) | (t == 0) & (core == 0))
        def _():
            x_hop(1, cx)

        @when(t == 2)
        def _():
            x_hop(1, xp, inner)
            x_hop(2, cx, edge)

        @when(t == 3)
        def _():
            x_hop(2, cx, inner)

        @when(t == 4)
        def _():
            x_hop(2, xp)

        @when(t == 6)
        def _():
            x_hop(3, cx)
            x_hop(3, xp)

        @when(t == 7)
        def _():
            x_late()

        @when(t == 9)
        def _():
            x_hop(1, xp, edge)

        lax.fori_loop(lead(t), lead(t + 1), partial_c, 0)

        @when((t == 0) & (core == 1))
        def _():
            x_from_partner()

        @when((t >= 1) & (t < 5))
        def _():
            rows = pl.ds(pl.multiple_of((t - 1) * width, width), width)
            pltpu.make_async_copy(w2_hbm.at[rows], w2.at[rows], ld.at[3]).start()

        @when(t == 5)
        def _():
            pltpu.make_async_copy(w2_hbm, w2, ld.at[3]).wait()

        def partial(m, carry):
            own_b = z * 4 + jnp.where(t == 6, m, t - 5)
            late = block(t - 3 - t // 16 + t // 17, cx)
            partial_z(jnp.where(t < 9, own_b, jnp.where(t < 11, away + 10 - t + 2 * m, late)))
            return carry

        two = (t == 6) | (t == 9) | (t == 10)
        lax.fori_loop(0, jnp.where(two, 2, jnp.where((t >= 6) & (t != 15), 1, 0)), partial, 0)

        @when(t == 16)
        def _():
            finish(0)
            pass_on_x(13)
            pass_on_x(14)
            partial_z(block(13, cx))

        @when(inner & (t == 12))
        def _():
            z_add(away + 0)

        @when((t >= 1) & (t < 13))
        def _():
            pass_on_y(t - 1)

        @when((t >= 2) & (t < 14))
        def _():
            pass_on_x(t - 2)

        @when(t == 15)
        def _():
            pass_on_y(13)
            pass_on_x(12)

            @when(inner)
            def _():
                z_add(block(10, cx))

            pass_on_y(14)

            @when(inner)
            def _():
                z_add(block(11, cx))

        @when(inner & ((t == 11) | (t == 12)))
        def _():
            z_add(away + 14 - t)

        @when(inner & ((t == 13) | (t == 14)))
        def _():
            z_add(block(t - 5, cx))

        @when(inner & (t == 13))
        def _():
            z_add(z * 4 + 1)
            z_add(z * 4 + 3)

        @when(inner & ((t == 14) | (t == 15)))
        def _():
            z_add(z * 4 + 2 * t - 28)

        @when(t >= 16)
        def _():
            finish(t - 15)

        return carry

    lax.fori_loop(0, BLOCKS + 4, step, 0)

    def collect(c, carry):
        t_a(c, c).wait_recv()
        return carry

    lax.fori_loop(0, 4, collect, 0)
    def gather_out():
        for c in range(4):
            out_ref[:, c * ab.shape[2]:(c + 1) * ab.shape[2]] = ab[c]

    gather_out()

    def sent_all(kind, ref, dev):
        rc(ref, ref, sent.at[kind], xr.at[0], dev).wait_send()

    def wait_sends():
        sent_all(0, xg.at[own], dev_x)
        sent_all(1, xg.at[pl.ds(0, 8)], dev_s)
        for k in range(4):
            @when(z == k)
            def _(k=k):
                if k < 3:
                    sent_all(2, xg.at[pl.ds(0, 2 * (k + 1))], dev_up)
                if k > 0:
                    sent_all(3, xg.at[pl.ds(0, 2 * (4 - k))], dev_dn)
        sent_all(4, crv, dev_y)
        sent_all(5, hg.at[pl.ds(0, 2)], dev_y)
        sent_all(6, hg.at[pl.ds(0, 4)], dev_x)
        sent_all(7, hg.at[pl.ds(0, 8)], dev_s)
        sent_all(8, zp.at[pl.ds(0, 12)], dev_y)
        sent_all(9, fb, dev_x)

    wait_sends()


def solution(mesh):
    def body(x, w1, w2):
        dma = pltpu.SemaphoreType.DMA
        bf, f32 = jnp.bfloat16, jnp.float32
        depth, width = w1.shape
        cols = w2.shape[1]
        return pl.pallas_call(
            kernel,
            out_shape=jax.ShapeDtypeStruct(x.shape, bf),
            in_specs=[pl.BlockSpec(memory_space=pltpu.HBM)] * 3,
            out_specs=pl.BlockSpec(memory_space=pltpu.VMEM),
            scratch_shapes=[
                pltpu.VMEM((BLOCKS, ROWS, depth), bf),
                pltpu.VMEM(w1.shape, bf),
                pltpu.VMEM(w2.shape, bf),
                pltpu.VMEM((BLOCKS, ROWS, width), f32),
                pltpu.VMEM((BLOCKS, HALF, width), f32),
                pltpu.VMEM((BLOCKS, 4, ROWS, width), bf),
                pltpu.VMEM((BLOCKS, ROWS, cols), f32),
                pltpu.VMEM((BLOCKS, ROWS, cols), f32),
                pltpu.VMEM((BLOCKS, ROWS, cols), f32),
                pltpu.VMEM((4, ROWS, cols), bf),
                pltpu.VMEM((4, ROWS, cols), bf),
                dma((4,)), dma((10,)),
            ] + [dma((BLOCKS,))] + [dma((8,))] * 4 + [dma((BLOCKS + 4,)), dma((4,))],
            compiler_params=pltpu.CompilerParams(
                collective_id=0, has_side_effects=True, vmem_limit_bytes=56_150_000),
        )(x, w1, w2)

    return jax.shard_map(
        body,
        mesh=mesh,
        in_specs=(P(("cx", "cz"), "cy"), P("cy", ("cz", "cx")), P("cz", ("cy", "cx"))),
        out_specs=P(("cx", "cz"), "cy"),
        check_vma=False,
    )
```

```python
import math

import jax
import jax.numpy as jnp
from jax import lax
from jax.experimental import pallas as pl
from jax.experimental.pallas import tpu as pltpu
from jax.sharding import PartitionSpec as P

MESH = pl.DeviceIdType.MESH
ROWS = 64
HALF = ROWS // 2
BLOCKS = 16


def kernel(x_hbm, w1_hbm, w2_hbm, out_ref, xg, w1, w2, cp, crv, hg, zp, zu, zd, fb, ab, ld,
           sent, xr, cr, hyr, hxr, dr, zr, ar):
    z, y, cx = lax.axis_index("cz"), lax.axis_index("cy"), lax.axis_index("cx")
    core = cx % 2
    xp = (cx + 2) % 4
    sib = cx + 1 - 2 * core
    dev_y = (z, 1 - y, cx)
    dev_x = (z, y, xp)
    dev_s = (z, y, sib)
    dev_up = ((z + 1) % 4, y, cx)
    dev_dn = ((z + 3) % 4, y, cx)
    width = w1.shape[1]
    left, right = pl.ds(0, width // 2), pl.ds(width // 2, width // 2)
    slot, slot_xp = core * 2 + cx // 2, core * 2 + 1 - cx // 2
    pair_sib = pl.ds((1 - core) * 2, 2)

    loads = [pltpu.make_async_copy(x_hbm, xg.at[z * 4 + cx], ld.at[0]),
             pltpu.make_async_copy(w1_hbm.at[:, left], w1.at[:, left], ld.at[1]),
             pltpu.make_async_copy(w1_hbm.at[:, right], w1.at[:, right], ld.at[2])]
    for load in loads:
        load.start()

    barrier = pltpu.get_barrier_semaphore()
    near = z + 1 - 2 * (z % 2)
    for dev in (dev_y, dev_x, dev_s, (near, y, xp), (near, y, sib), (near, y, (sib + 2) % 4)):
        pl.semaphore_signal(barrier, inc=1, device_id=dev, device_id_type=MESH)

    @pl.when(z < 3)
    def _():
        pl.semaphore_signal(barrier, inc=1, device_id=dev_up, device_id_type=MESH)

    @pl.when(z > 0)
    def _():
        pl.semaphore_signal(barrier, inc=1, device_id=dev_dn, device_id_type=MESH)

    edge = (z == 0) | (z == 3)

    inner = jnp.logical_not(edge)

    @pl.when(edge)
    def _():
        pl.semaphore_wait(barrier, 7)

    @pl.when(inner)
    def _():
        pl.semaphore_wait(barrier, 8)

    def rc(src, dst, ssem, rsem, dev):
        return pltpu.make_async_remote_copy(src_ref=src, dst_ref=dst, send_sem=ssem, recv_sem=rsem,
                                            device_id=dev, device_id_type=MESH)

    mine = pl.ds(pl.multiple_of(y * HALF, HALF), HALF)
    other = pl.ds(pl.multiple_of((1 - y) * HALF, HALF), HALF)

    def turn(b):
        p = b // 4
        return b % 4 + jnp.where((p == near) | (p == 2 - z // 2), 4, 0)

    def t_xx(b):
        return rc(xg.at[b], xg.at[b], sent.at[0], xr.at[b], dev_x)

    def t_xd(b):
        return rc(xg.at[b], xg.at[b], sent.at[1], xr.at[b], dev_s)

    def t_xu(b):
        return rc(xg.at[b], xg.at[b], sent.at[2], xr.at[b], dev_up)

    def t_xn(b):
        return rc(xg.at[b], xg.at[b], sent.at[3], xr.at[b], dev_dn)

    def t_c(b):
        return rc(cp.at[b, other], crv.at[b], sent.at[4], cr.at[turn(b)], dev_y)

    def t_hy(b, rows):
        return rc(hg.at[b, slot, rows], hg.at[b, slot, rows], sent.at[5], hyr.at[turn(b)], dev_y)

    def t_hx(b, rows):
        return rc(hg.at[b, slot, rows], hg.at[b, slot, rows], sent.at[6], hxr.at[turn(b)], dev_x)

    def t_hd(b, c):
        return rc(hg.at[b, c], hg.at[b, c], sent.at[7], dr.at[turn(b)], dev_s)

    def t_zu(b):
        return rc(zp.at[b], zu.at[b], sent.at[8], zr.at[b], dev_up)

    def t_zn(b, last):
        return rc(zp.at[b], zd.at[b], sent.at[8], zr.at[jnp.where(last, BLOCKS + b % 4, b)], dev_dn)

    def t_a(q, frm):
        return rc(fb.at[q], ab.at[frm], sent.at[9], ar.at[frm], (near, y, q))

    low = 1 - z // 2

    def plane(s):
        return jnp.where(s == 0, z, jnp.where(s == 1, 1 + low, jnp.where(s == 2, 3 * low, near)))

    def block(n, me):
        s, j = n // 4, n % 4
        chip = me // 2 * 2
        own_first = chip + jnp.where(s == 1, j + 1 - 2 * (j % 2), jnp.where(j < 2, (me + j) % 2, j))
        return plane(s) * 4 + jnp.where(s < 2, own_first % 4, j)

    def when(cond):
        return pl.when(cond)

    loads[0].wait()
    own = z * 4 + cx
    far = z * 4 + xp
    def x_line():
        @when(z < 3)
        def _():
            t_xu(own).start()

        @when(z > 0)
        def _():
            t_xn(own).start()

    @when(core == 0)
    def _():
        t_xx(own).start()

    @when(core == 1)
    def _():
        x_line()

    t_xd(own).start()

    def x_from_partner():
        t_xx(far).wait_recv()
        t_xd(far).start()

        @when(z < 2)
        def _():
            t_xu(far).start()

        @when(z > 1)
        def _():
            t_xn(far).start()

    def x_late():
        @when(z == 2)
        def _():
            t_xu(far).start()

        @when(z == 1)
        def _():
            t_xn(far).start()

    def x_hop(dist, c, where=True):
        @when((z >= dist) & where)
        def _():
            b = (z - dist) * 4 + c
            t_xu(b).wait_recv()
            t_xd(b).start()

            @when(z < 3)
            def _():
                t_xu(b).start()

        @when((z + dist < 4) & where)
        def _():
            b = (z + dist) * 4 + c
            t_xn(b).wait_recv()
            t_xd(b).start()

            @when(z > 0)
            def _():
                t_xn(b).start()

    def first_matmul(n):
        b = block(n, cx)

        @when((b + cx) % 2 == 1)
        def _():
            t_xd(b).wait_recv()

        cp[b] = jnp.dot(xg[b], w1[...], preferred_element_type=jnp.float32)
        t_c(b).start()

    def activation(n):
        b = block(n, cx)
        t_c(b).wait_recv()
        c = (cp[b, mine] + crv[b]).astype(jnp.bfloat16).astype(jnp.float32)
        t = jnp.tanh(math.sqrt(2 / math.pi) * (c + 0.044715 * (c * c * c)))
        hg[b, slot, mine] = (0.5 * c * (1.0 + t)).astype(jnp.bfloat16)
        t_hy(b, mine).start()
        t_hx(b, mine).start()

    def pass_on_y(n):
        b = block(n, cx)
        t_hy(b, other).wait_recv()
        t_hx(b, other).start()
        t_hd(b, slot).start()

    def pass_on_x(n):
        b = block(n, xp)
        piece = hg.at[b, slot_xp]
        rc(piece, piece, sent.at[6], hxr.at[turn(b)], dev_x).wait_recv()
        t_hd(b, slot_xp).start()

    def second_matmul(b):
        pieces = hg.at[b, pair_sib]
        rc(pieces, pieces, sent.at[7], dr.at[turn(b)], dev_s).wait_recv()
        acc = jnp.dot(hg[b, 0], w2[pl.ds(0, width)], preferred_element_type=jnp.float32)
        for i in range(1, 4):
            c = (i % 2) * 2 + i // 2
            acc += jnp.dot(hg[b, i], w2[pl.ds(c * width, width)], preferred_element_type=jnp.float32)
        zp[b] = acc

    def last_plane(b):
        p = b // 4
        return p + 1 - 2 * (p % 2)

    def z_send(b):
        @when(last_plane(b) > z)
        def _():
            t_zu(b).start()

        @when(last_plane(b) < z)
        def _():
            t_zn(b, last_plane(b) == z - 1).start()

    def z_add(b):
        @when(last_plane(b) > z)
        def _():
            t_zu(b).wait_recv()
            zp[b] += zu[b]

        @when(last_plane(b) < z)
        def _():
            t_zn(b, False).wait_recv()
            zp[b] += zd[b]

        z_send(b)

    def finish(q):
        b = near * 4 + q

        @when(z > 0)
        def _():
            t_zu(b).wait_recv()
            zp[b] += zu[b]

        @when(z < 3)
        def _():
            t_zn(b, True).wait_recv()
            zp[b] += zd[b]

        fb[q] = zp[b].astype(jnp.bfloat16)
        t_a(q, cx).start()

    for load, cols in ((loads[1], left), (loads[2], right)):
        load.wait()
        cp[own, :, cols] = jnp.dot(xg[own], w1[:, cols], preferred_element_type=jnp.float32)
        rc(cp.at[own, other, cols], crv.at[own, :, cols], sent.at[4], cr.at[turn(own)], dev_y).start()

    @when(core == 0)
    def _():
        x_line()

    @when(core == 1)
    def _():
        t_xx(own).start()

    first_matmul(1)

    def lead(t):
        return jnp.minimum(BLOCKS, t + 2 + jnp.clip(t - 11, 0, 1) + jnp.where((t == 0) & (core == 0) | (t < 0), 1, 0))

    def partial_c(n, carry):
        first_matmul(n)
        return carry

    def partial_z(b):
        second_matmul(b)

        @when(edge & (b // 4 != near))
        def _():
            z_send(b)

    away = plane(1) * 4

    def step(i, carry):
        t = i - 1

        @when(inner & (t == 11))
        def _():
            z_add(away + 1)

        @when(t == 15)
        def _():
            pass_on_y(12)

        @when((t >= 0) & (t < BLOCKS))
        def _():
            activation(t)

        @when(t == 16)
        def _():
            pass_on_y(15)

        @when(t == 17)
        def _():
            pass_on_x(15)

        @when((t < 0) & (core == 0))
        def _():
            x_from_partner()

        @when((t < 0) & (core == 1) | (t == 0) & (core == 0))
        def _():
            x_hop(1, cx)

        @when(t == 2)
        def _():
            x_hop(1, xp, inner)
            x_hop(2, cx, edge)

        @when(t == 3)
        def _():
            x_hop(2, cx, inner)

        @when(t == 4)
        def _():
            x_hop(2, xp)

        @when(t == 6)
        def _():
            x_hop(3, cx)
            x_hop(3, xp)

        @when(t == 7)
        def _():
            x_late()

        @when(t == 9)
        def _():
            x_hop(1, xp, edge)

        lax.fori_loop(lead(t), lead(t + 1), partial_c, 0)

        @when((t == 0) & (core == 1))
        def _():
            x_from_partner()

        @when((t >= 1) & (t < 5))
        def _():
            rows = pl.ds(pl.multiple_of((t - 1) * width, width), width)
            pltpu.make_async_copy(w2_hbm.at[rows], w2.at[rows], ld.at[3]).start()

        @when(t == 5)
        def _():
            pltpu.make_async_copy(w2_hbm, w2, ld.at[3]).wait()

        def partial(m, carry):
            own_b = z * 4 + jnp.where(t == 6, m, t - 5)
            late = block(t - 3 - t // 16 + t // 17, cx)
            partial_z(jnp.where(t < 9, own_b, jnp.where(t < 11, away + 10 - t + 2 * m, late)))
            return carry

        two = (t == 6) | (t == 9) | (t == 10)
        lax.fori_loop(0, jnp.where(two, 2, jnp.where((t >= 6) & (t != 15), 1, 0)), partial, 0)

        @when(t == 16)
        def _():
            finish(0)
            pass_on_x(13)
            pass_on_x(14)
            partial_z(block(13, cx))

        @when(inner & (t == 12))
        def _():
            z_add(away + 0)

        @when((t >= 1) & (t < 13))
        def _():
            pass_on_y(t - 1)

        @when((t >= 2) & (t < 14))
        def _():
            pass_on_x(t - 2)

        @when(t == 15)
        def _():
            pass_on_y(13)
            pass_on_x(12)

            @when(inner)
            def _():
                z_add(block(10, cx))

            pass_on_y(14)

            @when(inner)
            def _():
                z_add(block(11, cx))

        @when(inner & ((t == 11) | (t == 12)))
        def _():
            z_add(away + 14 - t)

        @when(inner & ((t == 13) | (t == 14)))
        def _():
            z_add(block(t - 5, cx))

        @when(inner & (t == 13))
        def _():
            z_add(z * 4 + 1)
            z_add(z * 4 + 3)

        @when(inner & ((t == 14) | (t == 15)))
        def _():
            z_add(z * 4 + 2 * t - 28)

        @when(t >= 16)
        def _():
            finish(t - 15)

        return carry

    lax.fori_loop(0, BLOCKS + 4, step, 0)

    def collect(c, carry):
        t_a(c, c).wait_recv()
        return carry

    lax.fori_loop(0, 4, collect, 0)
    def gather_out():
        for c in range(4):
            out_ref[:, c * ab.shape[2]:(c + 1) * ab.shape[2]] = ab[c]

    gather_out()

    def sent_all(kind, ref, dev):
        rc(ref, ref, sent.at[kind], xr.at[0], dev).wait_send()

    def wait_sends():
        sent_all(0, xg.at[own], dev_x)
        sent_all(1, xg.at[pl.ds(0, 8)], dev_s)
        for k in range(4):
            @when(z == k)
            def _(k=k):
                if k < 3:
                    sent_all(2, xg.at[pl.ds(0, 2 * (k + 1))], dev_up)
                if k > 0:
                    sent_all(3, xg.at[pl.ds(0, 2 * (4 - k))], dev_dn)
        sent_all(4, crv, dev_y)
        sent_all(5, hg.at[pl.ds(0, 2)], dev_y)
        sent_all(6, hg.at[pl.ds(0, 4)], dev_x)
        sent_all(7, hg.at[pl.ds(0, 8)], dev_s)
        sent_all(8, zp.at[pl.ds(0, 12)], dev_y)
        sent_all(9, fb, dev_x)

    wait_sends()


def solution(mesh):
    def body(x, w1, w2):
        dma = pltpu.SemaphoreType.DMA
        bf, f32 = jnp.bfloat16, jnp.float32
        depth, width = w1.shape
        cols = w2.shape[1]
        return pl.pallas_call(
            kernel,
            out_shape=jax.ShapeDtypeStruct(x.shape, bf),
            in_specs=[pl.BlockSpec(memory_space=pltpu.HBM)] * 3,
            out_specs=pl.BlockSpec(memory_space=pltpu.VMEM),
            scratch_shapes=[
                pltpu.VMEM((BLOCKS, ROWS, depth), bf),
                pltpu.VMEM(w1.shape, bf),
                pltpu.VMEM(w2.shape, bf),
                pltpu.VMEM((BLOCKS, ROWS, width), f32),
                pltpu.VMEM((BLOCKS, HALF, width), f32),
                pltpu.VMEM((BLOCKS, 4, ROWS, width), bf),
                pltpu.VMEM((BLOCKS, ROWS, cols), f32),
                pltpu.VMEM((BLOCKS, ROWS, cols), f32),
                pltpu.VMEM((BLOCKS, ROWS, cols), f32),
                pltpu.VMEM((4, ROWS, cols), bf),
                pltpu.VMEM((4, ROWS, cols), bf),
                dma((4,)), dma((10,)),
            ] + [dma((BLOCKS,))] + [dma((8,))] * 4 + [dma((BLOCKS + 4,)), dma((4,))],
            compiler_params=pltpu.CompilerParams(
                collective_id=0, has_side_effects=True, vmem_limit_bytes=56_150_000),
        )(x, w1, w2)

    return jax.shard_map(
        body,
        mesh=mesh,
        in_specs=(P(("cx", "cz"), "cy"), P("cy", ("cz", "cx")), P("cz", ("cy", "cx"))),
        out_specs=P(("cx", "cz"), "cy"),
        check_vma=False,
    )
```
